32 devices in a mesh: dp: 4 (over y, z), ep: 8 (over x, core).
Axes of the slice: x: 4, y: 2, z: 2, core: 2. Of those that a mesh axis runs over, the one named last changes fastest.
The devices are a block of a 4x4x8 slice.
Arguments:
- x: bfloat16 [16384, 4096], P(('dp', 'ep')), parts along dimension 0
- route_idx: int32 [16384, 2], P(('dp', 'ep')), parts along dimension 0
- gates: float32 [16384, 2], P(('dp', 'ep')), parts along dimension 0
- w1: bfloat16 [8, 4096, 6400], P('ep')
- w3: bfloat16 [8, 4096, 6400], P('ep')
- w2: bfloat16 [8, 6400, 4096], P('ep')
Outputs:
- output: bfloat16 [16384, 4096], P(('dp', 'ep')), parts along dimension 0
There are 4 independent parts. The reference program is written for one: setup_inputs(seed, part) draws one part's arguments, and reference() takes and returns one part's arrays. A program takes and returns all parts, laid end to end along the dimension named above; an argument that names none is the same for every part.
All inputs are finite; a program needn't handle non-finite values.
Results may differ from the reference program's by a relative error of at most 0.001.
Values are sent between devices in bfloat16 or wider.
A program may use at most 768 MiB of HBM per device.

```python
import jax
import jax.numpy as jnp
from jax import lax

D = 4096
FF = 6400
TOK = 512
EP = 8

T = EP * TOK
RB = TOK // 2
NB = 2 * T // RB + EP


def build_route(counts, key):
    ks, kp = jax.random.split(key)
    cum = jnp.cumsum(counts, axis=1)
    r = jnp.arange(TOK)
    s0 = jax.vmap(lambda c: jnp.searchsorted(c, r, side='right'))(cum)
    s1 = jnp.roll(s0, -(TOK // 2), axis=1)
    pairs = jnp.stack([s0, s1], axis=-1).astype(jnp.int32)
    swap = jax.random.bernoulli(ks, 0.5, (EP, TOK))
    pairs = jnp.where(swap[:, :, None], pairs[:, :, ::-1], pairs)
    keys = jax.random.split(kp, EP)
    pairs = jax.vmap(lambda k, p: jax.random.permutation(k, p, axis=0))(keys, pairs)
    return pairs.reshape(T, 2)


def setup_inputs(seed: int = 0, part: int = 0) -> dict:
    key = jax.random.fold_in(jax.random.key(seed), part)
    kx, kr, kg, kh, kc = jax.random.split(key, 5)
    kw1, kw3, kw2 = jax.random.split(jax.random.key(seed + 1), 3)
    x = jax.random.normal(kx, (T, D), jnp.float32).astype(jnp.bfloat16)
    dev = jnp.arange(EP)
    perm = jax.random.permutation(kh, EP)
    hot = perm[:3]
    cold = perm[3:]
    extra = jax.random.randint(kc, (EP, TOK // 4 - EP + 3), 0, EP - 3)
    cold_cnt = jnp.ones((EP, EP - 3), jnp.int32).at[dev[:, None], extra].add(1)
    counts = jnp.zeros((EP, EP), jnp.int32).at[:, cold].set(cold_cnt)
    amt = jnp.array([3 * TOK // 8, TOK // 4, TOK // 8], jnp.int32)
    hot_idx = hot[(jnp.arange(3)[None, :] + dev[:, None]) % 3]
    counts = counts.at[dev[:, None], hot_idx].set(jnp.broadcast_to(amt, (EP, 3)))
    route_idx = build_route(counts, kr)
    g0 = jax.random.uniform(kg, (T,), jnp.float32, 0.3, 0.7)
    gates = jnp.stack([g0, 1.0 - g0], axis=1)
    w1 = (jax.random.normal(kw1, (EP, D, FF), jnp.float32) * D ** -0.5).astype(jnp.bfloat16)
    w3 = (jax.random.normal(kw3, (EP, D, FF), jnp.float32) * D ** -0.5).astype(jnp.bfloat16)
    w2 = (jax.random.normal(kw2, (EP, FF, D), jnp.float32) * FF ** -0.5).astype(jnp.bfloat16)
    return {'x': x, 'route_idx': route_idx, 'gates': gates, 'w1': w1, 'w3': w3, 'w2': w2}


def reference(x, route_idx, gates, w1, w3, w2):
    e = route_idx.reshape(-1)
    g = gates.reshape(-1)
    tk = jnp.arange(2 * T, dtype=jnp.int32) // 2
    order = jnp.argsort(e, stable=True)
    se = e[order]
    counts = jnp.zeros((EP,), jnp.int32).at[e].add(1)
    start = jnp.cumsum(counts) - counts
    padded = (counts + RB - 1) // RB * RB
    pend = jnp.cumsum(padded)
    pstart = pend - padded
    dest = pstart[se] + jnp.arange(2 * T, dtype=jnp.int32) - start[se]
    tbuf = jnp.full((NB * RB,), T, jnp.int32).at[dest].set(tk[order])
    gbufv = jnp.zeros((NB * RB,), jnp.float32).at[dest].set(g[order])
    bexp = jnp.minimum(jnp.searchsorted(pend, jnp.arange(NB) * RB, side='right'), EP - 1)
    xe = jnp.concatenate([x, jnp.zeros((1, D), x.dtype)], axis=0)

    def step(y, blk):
        tb, gb, be = blk
        rows = xe[tb]
        a = jnp.dot(rows, w1[be], preferred_element_type=jnp.float32)
        b = jnp.dot(rows, w3[be], preferred_element_type=jnp.float32)
        h = (jax.nn.silu(a) * b).astype(jnp.bfloat16)
        o = jnp.dot(h, w2[be], preferred_element_type=jnp.float32).astype(jnp.bfloat16)
        return y.at[tb].add(gb[:, None] * o.astype(jnp.float32)), None

    y, _ = lax.scan(step, jnp.zeros((T + 1, D), jnp.float32),
                    (tbuf.reshape(NB, RB), gbufv.reshape(NB, RB), bexp))
    return y[:T].astype(jnp.bfloat16)
```

```python
import functools

import jax
import jax.numpy as jnp
from jax import lax
from jax.experimental import pallas as pl
from jax.experimental.pallas import tpu as pltpu
from jax.sharding import PartitionSpec as P

CHUNKS = (96, 128, 144, 144)
TN = 256
WIN = 256
SIZES = (4, 8, 9, 10)
TD = 256


def row_tiles(n, rows, body):
    sizes = [(rows * k + 255) // 256 * 16 for k in SIZES]
    step = rows // 2
    nbig = jnp.maximum(n - sizes[-1] + step - 1, 0) // step

    def big(i, _):
        body(pl.multiple_of(i * step, 16), step)
        return 0

    lax.fori_loop(0, nbig, big, 0)
    off = pl.multiple_of(nbig * step, 16)
    rest = n - off
    low = 0
    for size in sizes:
        pl.when((rest > low) & (rest <= size))(functools.partial(body, off, size))
        low = size


def ffn_kernel(base_ref, dl_ref, dc_ref, x_hbm, w1_hbm, w3_hbm, w2_hbm, o_hbm,
               xg, xc, h, up, down, oc, sel, obuf, x_sem, up_sem, down_sem, o_sem):
    nb, tok = dl_ref.shape
    d = xg.shape[1]
    ff = h.shape[1]
    nup = ff // TN
    ndown = d // TD
    n = base_ref[nb]

    def up_copies(i):
        slot = lax.rem(i, 2)
        cols = pl.ds(pl.multiple_of(i * TN, TN), TN)
        return [pltpu.make_async_copy(src.at[:, cols], up.at[slot, k], up_sem.at[slot, k])
                for k, src in enumerate((w1_hbm, w3_hbm))]

    def down_copies(i):
        slot = lax.rem(i, 2)
        cols = pl.ds(pl.multiple_of(i * TD, TD), TD)
        return [pltpu.make_async_copy(w2_hbm.at[:, cols], down.at[slot], down_sem.at[slot])]

    def start(copies):
        for copy in copies:
            copy.start()

    def wait(copies):
        for copy in copies:
            copy.wait()

    def out_copy(i):
        slot = lax.rem(i, 2)
        return pltpu.make_async_copy(obuf.at[slot], o_hbm.at[:, pl.ds(pl.multiple_of(i * TD, TD), TD)],
                                     o_sem.at[slot])

    x_copy = pltpu.make_async_copy(x_hbm, xg, x_sem)
    x_copy.start()
    start(up_copies(0))
    start(down_copies(0))
    oc[...] = jnp.zeros_like(oc)
    for b in range(nb):
        al = (base_ref[b] // 16) * 16
        k = lax.broadcasted_iota(jnp.int32, (tok, WIN), 1)
        sel[pl.ds(b * tok, tok), :] = jnp.where(dc_ref[pl.ds(b * tok, tok), :] - al == k, 1.0, 0.0).astype(sel.dtype)
    x_copy.wait()

    for b in range(nb):
        base = base_ref[b]
        al = pl.multiple_of((base // 16) * 16, 16)
        r = lax.broadcasted_iota(jnp.int32, (WIN, tok), 0)
        p = jnp.where(dl_ref[b:b + 1, :] - al == r, 1.0, 0.0).astype(xg.dtype)
        new = jnp.dot(p, xg[pl.ds(b * tok, tok), :], preferred_element_type=jnp.float32).astype(xc.dtype)
        if b == 0:
            xc[pl.ds(0, WIN), :] = new
        else:
            keep = lax.broadcasted_iota(jnp.int32, (16, d), 0) < base - al
            old = xc[pl.ds(al, 16), :].astype(jnp.float32)
            head = jnp.where(keep, old, new[:16].astype(jnp.float32)).astype(xc.dtype)
            xc[pl.ds(al, 16), :] = head
            xc[pl.ds(al + 16, WIN - 16), :] = new[16:]

    def up_step(i, _):
        slot = lax.rem(i, 2)
        wait(up_copies(i))

        @pl.when(i + 1 < nup)
        def _():
            start(up_copies(i + 1))

        def body(off, size):
            rows = xc[pl.ds(off, size), :]
            a = jnp.dot(rows, up[slot, 0], preferred_element_type=jnp.float32)
            b = jnp.dot(rows, up[slot, 1], preferred_element_type=jnp.float32)
            h[pl.ds(off, size), pl.ds(pl.multiple_of(i * TN, TN), TN)] = (jax.nn.silu(a) * b).astype(h.dtype)

        row_tiles(n, h.shape[0], body)
        return 0

    lax.fori_loop(0, nup, up_step, 0)

    def down_step(i, _):
        slot = lax.rem(i, 2)
        wait(down_copies(i))

        @pl.when(i + 1 < ndown)
        def _():
            start(down_copies(i + 1))

        @pl.when(i >= 2)
        def _():
            out_copy(i - 2).wait()

        def body(off, size):
            oc[pl.ds(off, size), :] = jnp.dot(h[pl.ds(off, size), :], down[slot],
                                              preferred_element_type=jnp.float32).astype(oc.dtype)

        row_tiles(n, h.shape[0], body)
        for b in range(nb):
            al = pl.multiple_of((base_ref[b] // 16) * 16, 16)
            obuf[slot, pl.ds(b * tok, tok), :] = jnp.dot(
                sel[pl.ds(b * tok, tok), :], oc[pl.ds(al, WIN), :],
                preferred_element_type=jnp.float32).astype(obuf.dtype)
        out_copy(i).start()
        return 0

    lax.fori_loop(0, ndown, down_step, 0)
    out_copy(ndown - 2).wait()
    out_copy(ndown - 1).wait()


def expert_rows(base, dl, x, w1, w3, w2):
    nb, tok = dl.shape
    rows, d = x.shape
    ff = w1.shape[1]
    bf = jnp.bfloat16
    smem = pl.BlockSpec(memory_space=pltpu.SMEM)
    vmem = pl.BlockSpec(memory_space=pltpu.VMEM)
    hbm = pl.BlockSpec(memory_space=pl.ANY)
    return pl.pallas_call(
        ffn_kernel,
        out_shape=jax.ShapeDtypeStruct((rows, d), x.dtype),
        in_specs=[smem, vmem, vmem, hbm, hbm, hbm, hbm],
        out_specs=hbm,
        scratch_shapes=[
            pltpu.VMEM((rows, d), bf),
            pltpu.VMEM((rows + WIN, d), bf),
            pltpu.VMEM((rows, ff), bf),
            pltpu.VMEM((2, 2, d, TN), bf),
            pltpu.VMEM((2, ff, TD), bf),
            pltpu.VMEM((rows + WIN, TD), bf),
            pltpu.VMEM((rows, WIN), bf),
            pltpu.VMEM((2, rows, TD), bf),
            pltpu.SemaphoreType.DMA,
            pltpu.SemaphoreType.DMA((2, 2)),
            pltpu.SemaphoreType.DMA((2,)),
            pltpu.SemaphoreType.DMA((2,)),
        ],
        compiler_params=pltpu.CompilerParams(vmem_limit_bytes=66000000),
        cost_estimate=pl.CostEstimate(flops=rows * d * ff * 3, transcendentals=rows * ff,
                                      bytes_accessed=3 * d * ff * 2 + 4 * rows * d),
        name='ffn',
    )(base, dl, dl.reshape(rows, 1), x, w1, w3, w2)


def solution(mesh):
    ep = mesh.shape['ep']

    def local(x, route_idx, gates, w1, w3, w2):
        tok, d = x.shape
        me = lax.axis_index('ep')
        ids = lax.all_gather(route_idx, 'ep')
        hit = jnp.any(ids == me, axis=2)
        table = jnp.sum(jnp.where(route_idx[:, :, None] == jnp.arange(ep, dtype=route_idx.dtype),
                                  gates[:, :, None], 0.0), axis=1)
        t = jnp.arange(tok)
        first = jnp.zeros((tok,), jnp.int32)
        starts = []
        for size in CHUNKS:
            starts.append(sum(CHUNKS[:len(starts)]))
            first = jnp.where(t >= starts[-1], starts[-1], first)
        low = ((t[:, None] < t[None, :]) & (t[:, None] >= first[None, :])).astype(jnp.bfloat16)
        before = jnp.dot(hit.astype(jnp.bfloat16), low, preferred_element_type=jnp.float32).astype(jnp.int32)
        hits = hit.astype(jnp.int32)
        ys = []
        for s, size in zip(starts, CHUNKS):
            part = slice(s, s + size)
            total = jnp.cumsum(jnp.sum(hits[:, part], axis=1))
            base = jnp.concatenate([jnp.zeros((1,), jnp.int32), total])
            dest = jnp.where(hit[:, part], before[:, part] + base[:ep, None], -1)
            xs = lax.all_gather(x[part], 'ep').reshape(ep * size, d)
            o = expert_rows(base, dest, xs, w1[0], w3[0], w2[0])
            back = lax.all_to_all(o.reshape(ep, size, d), 'ep', 0, 0, tiled=True)
            g = table[part]
            y = g[:, 0:1] * back[0].astype(jnp.float32)
            for j in range(1, ep):
                y = y + g[:, j:j + 1] * back[j].astype(jnp.float32)
            ys.append(y.astype(x.dtype))
        return jnp.concatenate(ys, axis=0)

    spec = P(('dp', 'ep'), None)
    wspec = P('ep', None, None)
    return jax.shard_map(local, mesh=mesh, in_specs=(spec, spec, spec, wspec, wspec, wspec),
                         out_specs=spec, check_vma=False)
```

```python
import functools

import jax
import jax.numpy as jnp
from jax import lax
from jax.experimental import pallas as pl
from jax.experimental.pallas import tpu as pltpu
from jax.sharding import PartitionSpec as P


CHUNKS = (144, 144, 128, 96)
TN = 256
WIN = 256
SIZES = (4, 8, 9, 10)
TD = 256


def row_tiles(n, rows, body):
    sizes = [rows * k // 256 * 16 for k in SIZES]
    step = rows // 2
    nbig = jnp.maximum(n - sizes[-1] + step - 1, 0) // step

    def big(i, _):
        body(pl.multiple_of(i * step, 16), step)
        return 0

    lax.fori_loop(0, nbig, big, 0)
    off = pl.multiple_of(nbig * step, 16)
    rest = n - off
    low = 0
    for size in sizes:
        pl.when((rest > low) & (rest <= size))(functools.partial(body, off, size))
        low = size


def ffn_kernel(base_ref, dl_ref, dc_ref, x_hbm, w1_hbm, w3_hbm, w2_hbm, o_hbm,
               xg, xc, h, up, down, oc, sel, obuf, x_sem, up_sem, down_sem, o_sem):
    nb, tok = dl_ref.shape
    d = xg.shape[1]
    ff = h.shape[1]
    nup = ff // TN
    ndown = d // TD
    n = base_ref[nb]

    def up_copies(i):
        slot = lax.rem(i, 2)
        cols = pl.ds(pl.multiple_of(i * TN, TN), TN)
        return [pltpu.make_async_copy(src.at[:, cols], up.at[slot, k], up_sem.at[slot, k])
                for k, src in enumerate((w1_hbm, w3_hbm))]

    def down_copies(i):
        slot = lax.rem(i, 2)
        cols = pl.ds(pl.multiple_of(i * TD, TD), TD)
        return [pltpu.make_async_copy(w2_hbm.at[:, cols], down.at[slot], down_sem.at[slot])]

    def start(copies):
        for copy in copies:
            copy.start()

    def wait(copies):
        for copy in copies:
            copy.wait()

    def out_copy(i):
        slot = lax.rem(i, 2)
        return pltpu.make_async_copy(obuf.at[slot], o_hbm.at[:, pl.ds(pl.multiple_of(i * TD, TD), TD)],
                                     o_sem.at[slot])

    x_copies = [pltpu.make_async_copy(x_hbm.at[pl.ds(b * tok, tok)], xg.at[pl.ds(b * tok, tok)], x_sem.at[b])
                for b in range(nb)]
    start(x_copies)
    start(up_copies(0))
    start(down_copies(0))
    oc[...] = jnp.zeros_like(oc)
    for b in range(nb):
        al = (base_ref[b] // 16) * 16
        k = lax.broadcasted_iota(jnp.int32, (tok, WIN), 1)
        sel[pl.ds(b * tok, tok), :] = jnp.where(dc_ref[pl.ds(b * tok, tok), :] - al == k, 1.0, 0.0).astype(sel.dtype)

    for b in range(nb):
        x_copies[b].wait()
        base = base_ref[b]
        al = pl.multiple_of((base // 16) * 16, 16)
        r = lax.broadcasted_iota(jnp.int32, (WIN, tok), 0)
        p = jnp.where(dl_ref[b:b + 1, :] - al == r, 1.0, 0.0).astype(xg.dtype)
        new = jnp.dot(p, xg[pl.ds(b * tok, tok), :], preferred_element_type=jnp.float32).astype(xc.dtype)
        if b == 0:
            xc[pl.ds(0, WIN), :] = new
        else:
            keep = lax.broadcasted_iota(jnp.int32, (16, d), 0) < base - al
            old = xc[pl.ds(al, 16), :].astype(jnp.float32)
            head = jnp.where(keep, old, new[:16].astype(jnp.float32)).astype(xc.dtype)
            xc[pl.ds(al, 16), :] = head
            xc[pl.ds(al + 16, WIN - 16), :] = new[16:]

    def up_step(i, _):
        slot = lax.rem(i, 2)
        wait(up_copies(i))

        @pl.when(i + 1 < nup)
        def _():
            start(up_copies(i + 1))

        def body(off, size):
            rows = xc[pl.ds(off, size), :]
            a = jnp.dot(rows, up[slot, 0], preferred_element_type=jnp.float32)
            b = jnp.dot(rows, up[slot, 1], preferred_element_type=jnp.float32)
            h[pl.ds(off, size), pl.ds(pl.multiple_of(i * TN, TN), TN)] = (jax.nn.silu(a) * b).astype(h.dtype)

        row_tiles(n, h.shape[0], body)
        return 0

    lax.fori_loop(0, nup, up_step, 0)

    def down_step(i, _):
        slot = lax.rem(i, 2)
        wait(down_copies(i))

        @pl.when(i + 1 < ndown)
        def _():
            start(down_copies(i + 1))

        @pl.when(i >= 2)
        def _():
            out_copy(i - 2).wait()

        def body(off, size):
            oc[pl.ds(off, size), :] = jnp.dot(h[pl.ds(off, size), :], down[slot],
                                              preferred_element_type=jnp.float32).astype(oc.dtype)

        row_tiles(n, h.shape[0], body)
        for b in range(nb):
            al = pl.multiple_of((base_ref[b] // 16) * 16, 16)
            obuf[slot, pl.ds(b * tok, tok), :] = jnp.dot(
                sel[pl.ds(b * tok, tok), :], oc[pl.ds(al, WIN), :],
                preferred_element_type=jnp.float32).astype(obuf.dtype)
        out_copy(i).start()
        return 0

    lax.fori_loop(0, ndown, down_step, 0)
    out_copy(ndown - 2).wait()
    out_copy(ndown - 1).wait()


def expert_rows(base, dl, x, w1, w3, w2):
    nb, _ = dl.shape
    rows, d = x.shape
    ff = w1.shape[1]
    bf = jnp.bfloat16
    smem = pl.BlockSpec(memory_space=pltpu.SMEM)
    vmem = pl.BlockSpec(memory_space=pltpu.VMEM)
    hbm = pl.BlockSpec(memory_space=pl.ANY)
    return pl.pallas_call(
        ffn_kernel,
        out_shape=jax.ShapeDtypeStruct((rows, d), x.dtype),
        in_specs=[smem, vmem, vmem, hbm, hbm, hbm, hbm],
        out_specs=hbm,
        scratch_shapes=[
            pltpu.VMEM((rows, d), bf),
            pltpu.VMEM((rows + WIN, d), bf),
            pltpu.VMEM((rows, ff), bf),
            pltpu.VMEM((2, 2, d, TN), bf),
            pltpu.VMEM((2, ff, TD), bf),
            pltpu.VMEM((rows + WIN, TD), bf),
            pltpu.VMEM((rows, WIN), bf),
            pltpu.VMEM((2, rows, TD), bf),
            pltpu.SemaphoreType.DMA((nb,)),
            pltpu.SemaphoreType.DMA((2, 2)),
            pltpu.SemaphoreType.DMA((2,)),
            pltpu.SemaphoreType.DMA((2,)),
        ],
        compiler_params=pltpu.CompilerParams(vmem_limit_bytes=66000000),
        cost_estimate=pl.CostEstimate(flops=rows * d * ff * 3, transcendentals=rows * ff,
                                      bytes_accessed=3 * d * ff * 2 + 4 * rows * d),
        name='ffn',
    )(base, dl, dl.reshape(rows, 1), x, w1, w3, w2)


def solution(mesh):
    ep = mesh.shape['ep']

    def local(x, route_idx, gates, w1, w3, w2):
        tok, d = x.shape
        me = lax.axis_index('ep')
        ids = lax.all_gather(route_idx, 'ep')
        hit = jnp.any(ids == me, axis=2)
        table = jnp.sum(jnp.where(route_idx[:, :, None] == jnp.arange(ep, dtype=route_idx.dtype),
                                  gates[:, :, None], 0.0), axis=1)
        t = jnp.arange(tok)
        first = jnp.zeros((tok,), jnp.int32)
        starts = []
        for size in CHUNKS:
            starts.append(sum(CHUNKS[:len(starts)]))
            first = jnp.where(t >= starts[-1], starts[-1], first)
        low = ((t[:, None] < t[None, :]) & (t[:, None] >= first[None, :])).astype(jnp.bfloat16)
        before = jnp.dot(hit.astype(jnp.bfloat16), low, preferred_element_type=jnp.float32).astype(jnp.int32)
        hits = hit.astype(jnp.int32)
        outs = []
        for s, size in zip(starts, CHUNKS):
            part = slice(s, s + size)
            total = jnp.cumsum(jnp.sum(hits[:, part], axis=1))
            base = jnp.concatenate([jnp.zeros((1,), jnp.int32), total])
            dest = jnp.where(hit[:, part], before[:, part] + base[:ep, None], -1)
            xs = lax.all_gather(x[part], 'ep').reshape(ep * size, d)
            outs.append(expert_rows(base, dest, xs, w1[0], w3[0], w2[0]))
        ys = []
        for s, size, o in zip(starts, CHUNKS, outs):
            back = lax.all_to_all(o.reshape(ep, size, d), 'ep', 0, 0, tiled=True)
            g = table[s:s + size]
            y = g[:, 0:1] * back[0].astype(jnp.float32)
            for j in range(1, ep):
                y = y + g[:, j:j + 1] * back[j].astype(jnp.float32)
            ys.append(y.astype(x.dtype))
        return jnp.concatenate(ys, axis=0)

    spec = P(('dp', 'ep'), None)
    wspec = P('ep', None, None)
    return jax.shard_map(local, mesh=mesh, in_specs=(spec, spec, spec, wspec, wspec, wspec),
                         out_specs=spec, check_vma=False)
```
